128 devices in a mesh: dp: 8 (over z, core), tp: 16 (over y, x).
Axes of the slice: x: 4, y: 4, z: 4, core: 2. Of those that a mesh axis runs over, the one named last changes fastest.
Arguments:
- head_fsdp: bfloat16 [4096, 128256], P(('dp', 'tp')), may hold values from -0.5 to 0.5
- hidden: bfloat16 [2048, 4096], P(('dp', 'tp')), may hold values from -48 to 48
- targets: int32 [2048], P(('dp', 'tp')), may hold values from 0 to 128255
Outputs:
- head_tp: bfloat16 [4096, 128256], P('dp', 'tp')
- log_norm: float32 [2048], P(('dp', 'tp'))
- target_logprob: float32 [2048], P(('dp', 'tp'))
The draws below stay inside these ranges and needn't reach their ends.
All inputs are finite; a program needn't handle non-finite values.
Results may differ from the reference program's by a relative error of at most 0.0004.
Values may be sent and summed in bfloat16 or wider, within the bound.
No kernel may reach another device: no remote copies, remote signals or barrier semaphores. Data moves between devices by JAX's collectives and lax.ppermute only.
A program may use at most 192 MiB of HBM per device.

```python
import jax
import jax.numpy as jnp
from jax import lax

D = 4096
V = 128256
SEQS = 256
BATCH = 2048
N_DP = 8


def draw_head_fsdp(key, part):
    values = jax.random.normal(jax.random.fold_in(key, 1), (D, V), jnp.float32)
    values = jnp.clip(values, -6.0, 6.0) * D ** (-0.5)
    return jnp.clip(values, -0.5, 0.5).astype(jnp.bfloat16)


def draw_hidden(key, part):
    noise = jnp.clip(jax.random.normal(jax.random.fold_in(key, 2), (BATCH, D), jnp.float32), -6.0, 6.0)
    values = 3.5 * noise
    return jnp.clip(values, -48.0, 48.0).astype(jnp.bfloat16)


def with_ends(drawn, own_key, smallest, largest):
    longest = drawn.shape.index(max(drawn.shape))
    spots = []
    for shift in (0, 1):
        where = [jax.random.randint(jax.random.fold_in(own_key, axis), (), 0, length) for axis, length in enumerate(drawn.shape)]
        where[longest] = (where[longest] + shift) % drawn.shape[longest]
        spots.append(tuple(where))
    return drawn.at[spots[0]].set(smallest).at[spots[1]].set(largest)


def setup_inputs(seed: int = 0) -> dict:
    arg_keys = jax.random.split(jax.random.key(seed), 4)
    return {
        "head_fsdp": draw_head_fsdp(jax.random.fold_in(arg_keys[3], 71), 0),
        "hidden": draw_hidden(jax.random.fold_in(arg_keys[3], 71), 0),
        "targets": with_ends(jax.random.randint(arg_keys[2], (BATCH,), 0, V), jax.random.fold_in(arg_keys[2], 1), 0, V - 1).astype(jnp.int32),
    }


def reference(head_fsdp, hidden, targets):
    hidden_blocks = hidden.reshape(N_DP, SEQS, D)
    target_blocks = targets.reshape(N_DP, SEQS)

    def score(pair):
        rows_hidden, rows_target = pair
        logits = jnp.dot(rows_hidden, head_fsdp, preferred_element_type=jnp.float32)
        top_logit = jnp.max(logits, axis=1)
        log_norm = top_logit + jnp.log(jnp.sum(jnp.exp(logits - top_logit[:, None]), axis=1))
        picked = jnp.take_along_axis(logits, rows_target[:, None].astype(jnp.int32), axis=1)[:, 0]
        return log_norm, picked - log_norm

    log_norm, logprob = lax.map(score, (hidden_blocks, target_blocks))
    return head_fsdp, log_norm.reshape(BATCH), logprob.reshape(BATCH)
```

```python
import jax
import jax.numpy as jnp
from jax import lax
from jax.experimental import pallas as pl
from jax.experimental.pallas import tpu as pltpu
from jax.sharding import Mesh
from jax.sharding import PartitionSpec as P

AXES = ("z", "c", "y", "x")
ROWS = 32
BLOCK = 8016
TP = 16
WIDTHS = (3072, 3072, 2048)
STARTS = (0, 3072, 6144)
GROUPS = (1, 1, 1)
D = 4096
LANES = 128
NEG = -3.0e38


def any_spec():
    return pl.BlockSpec(memory_space=pl.ANY)


def cut_body(off, width, head, out, buf, made, sem, gone):
    total = head.shape[1]
    plan = []
    for t in range(TP):
        start = t * BLOCK + off
        base = start // LANES * LANES
        end = min(-(-(start + width) // LANES) * LANES, total)
        plan.append((start - base, base, end - base))
    copies = [
        pltpu.make_async_copy(head.at[:, pl.ds(base, span)], buf.at[t, :, pl.ds(0, span)], sem.at[t])
        for t, (_, base, span) in enumerate(plan)
    ]
    sends = [pltpu.make_async_copy(made.at[t], out.at[t], gone.at[t]) for t in range(TP)]
    for c in copies:
        c.start()
    for t, (shift, _, span) in enumerate(plan):
        copies[t].wait()
        have = min(width, span - shift)
        whole = buf[t, :, :span]
        if shift:
            whole = pltpu.roll(whole, span - shift, 1)
        if have == width:
            made[t] = whole[:, :width]
        else:
            low = have // LANES * LANES
            made[t, :, :low] = whole[:, :low]
            tail = whole[:, low : low + LANES]
            lane = lax.broadcasted_iota(jnp.int32, tail.shape, 1)
            made[t, :, low : low + LANES] = jnp.where(lane < have - low, tail, jnp.zeros_like(tail))
            if low + LANES < width:
                made[t, :, low + LANES :] = jnp.zeros((ROWS, width - low - LANES), out.dtype)
        sends[t].start()
    for s in sends:
        s.wait()


def cut(head, off, width):
    return pl.pallas_call(
        lambda *refs: cut_body(off, width, *refs),
        out_shape=jax.ShapeDtypeStruct((TP, ROWS, width), head.dtype),
        in_specs=[pl.BlockSpec(memory_space=pltpu.HBM)],
        out_specs=pl.BlockSpec(memory_space=pltpu.HBM),
        scratch_shapes=[
            pltpu.VMEM((TP, ROWS, width + LANES), head.dtype),
            pltpu.VMEM((TP, ROWS, width), head.dtype),
            pltpu.SemaphoreType.DMA((TP,)),
            pltpu.SemaphoreType.DMA((TP,)),
        ],
    )(head)


def join_body(targets, hidden, out):
    out[:, :D] = hidden[...]
    row = lax.broadcasted_iota(jnp.int32, (16, LANES), 0)
    lane = lax.broadcasted_iota(jnp.int32, (16, LANES), 1)
    digits = jnp.zeros((16, LANES), jnp.int32)
    for r in range(16):
        value = targets[r]
        for place, digit in enumerate((value & 255, (value >> 8) & 255, value >> 16)):
            digits = jnp.where((row == r) & (lane == place), digit, digits)
    out[:, D:] = digits.astype(jnp.float32).astype(out.dtype)


def join(hidden, targets):
    return pl.pallas_call(
        join_body,
        out_shape=jax.ShapeDtypeStruct((16, D + LANES), hidden.dtype),
        in_specs=[pl.BlockSpec(memory_space=pltpu.SMEM), pl.BlockSpec(memory_space=pltpu.VMEM)],
        out_specs=pl.BlockSpec(memory_space=pltpu.VMEM),
        name="join",
    )(targets, hidden)


def turn(got, old, z, off):
    rows, width = got.shape
    part = width // 4
    valid = min(width, BLOCK - off)
    last = valid - 3 * part
    order = (1, 3, 2, 0)

    def body(info, got, *refs):
        refs = refs if old is None else refs[1:]
        head, *pieces = refs[:5]
        buf, made, sem, gone, kept = refs[5:]
        places = [lax.rem(info[0] + j, 4) for j in range(4)]
        copies = [
            pltpu.make_async_copy(
                got.at[:, pl.ds(pl.multiple_of(places[j] * part, LANES), part)], buf.at[j], sem.at[j]
            )
            for j in range(4)
        ]
        for j in order:
            copies[j].start()
        sends, keeps = [], []
        for j in order:
            copies[j].wait()
            made[j] = buf[j].T
            send = pltpu.make_async_copy(made.at[j], pieces[j], gone.at[j])
            send.start()
            sends.append(send)
            to = off + pl.multiple_of(places[j] * part, LANES)
            if last == part:
                keep = pltpu.make_async_copy(made.at[j], head.at[pl.ds(to, part), :], kept.at[j])
                keep.start()
                keeps.append(keep)
            else:
                full = pltpu.make_async_copy(made.at[j], head.at[pl.ds(to, part), :], kept.at[j])
                some = pltpu.make_async_copy(
                    made.at[j, pl.ds(0, last), :], head.at[pl.ds(off + 3 * part, last), :], kept.at[j]
                )
                pl.when(places[j] != 3)(full.start)
                pl.when(places[j] == 3)(some.start)
                keeps.append((places[j], full, some))
        for send in sends:
            send.wait()
        for keep in keeps:
            if last == part:
                keep.wait()
            else:
                pl.when(keep[0] != 3)(keep[1].wait)
                pl.when(keep[0] == 3)(keep[2].wait)

    return pl.pallas_call(
        body,
        in_specs=[pl.BlockSpec(memory_space=pltpu.SMEM), any_spec()] + ([] if old is None else [any_spec()]),
        out_specs=[any_spec()] * 5,
        out_shape=[jax.ShapeDtypeStruct((BLOCK, rows), got.dtype)]
        + [jax.ShapeDtypeStruct((part, rows), got.dtype)] * 4,
        scratch_shapes=[
            pltpu.VMEM((4, rows, part), got.dtype),
            pltpu.VMEM((4, part, rows), got.dtype),
            pltpu.SemaphoreType.DMA((4,)),
            pltpu.SemaphoreType.DMA((4,)),
            pltpu.SemaphoreType.DMA((4,)),
        ],
        input_output_aliases={} if old is None else {2: 0},
    )(z, got, *([] if old is None else [old]))


STEPS = 8
SLAB = D // STEPS
HALF = 512
QUARTER = 128


def score_body(plan, first, info, hid, *refs):
    count = len(plan)
    weights, refs = refs[: count * STEPS], refs[count * STEPS :]
    old = None
    if not first:
        old, refs = refs[0], refs[1:]
    new, logit, sem = refs[:3]
    tables = refs[3:]
    m = hid.shape[0]
    loads = [
        [
            pltpu.make_async_copy(
                weights[g * STEPS + j],
                tables[g].at[:, pl.ds(pl.multiple_of(info[j] * SLAB, SLAB), SLAB)],
                sem.at[g * STEPS + j],
            )
            for j in range(STEPS)
        ]
        for g in range(count)
    ]

    for load in loads[0]:
        load.start()
    for group in loads[1:]:
        for load in group:
            load.start()
    for g, (width, masked) in enumerate(plan):
        start, limit = info[STEPS + 2 * g], info[STEPS + 2 * g + 1]
        for load in loads[g]:
            load.wait()

        def half(i, done):
            logit[:, :width] = lax.dot_general(
                hid[pl.ds(pl.multiple_of(i * HALF, HALF), HALF), :D],
                tables[g][...],
                (((1,), (1,)), ((), ())),
                preferred_element_type=jnp.float32,
            )

            def stats(b, carry):
                at = pl.multiple_of(b * QUARTER, QUARTER)
                to = pl.multiple_of(i * HALF + b * QUARTER, QUARTER)
                logits = logit[pl.ds(at, QUARTER), :width]
                digits = hid[pl.ds(to, QUARTER), D:].astype(jnp.int32)
                target = digits[:, 0:1] + digits[:, 1:2] * 256 + digits[:, 2:3] * 65536 - start
                target = jnp.where(target < limit, target, -1)
                column = lax.broadcasted_iota(jnp.int32, logits.shape, 1)
                pick = jnp.sum(jnp.where(column == target, logits, 0.0), axis=1, keepdims=True)
                if masked:
                    logits = jnp.where(column < limit, logits, NEG)
                peak = jnp.max(logits, axis=1, keepdims=True)
                merge = not first or g > 0
                if merge:
                    before = (old if g == 0 else new)[pl.ds(to, QUARTER), :]
                    peak = jnp.maximum(peak, before[:, 0:1])
                mass = jnp.sum(jnp.exp(logits - peak), axis=1, keepdims=True)
                if merge:
                    mass = mass + before[:, 1:2] * jnp.exp(before[:, 0:1] - peak)
                    pick = pick + before[:, 2:3]
                lane = lax.broadcasted_iota(jnp.int32, (QUARTER, LANES), 1)
                new[pl.ds(to, QUARTER), :] = jnp.where(lane == 0, peak, jnp.where(lane == 1, mass, pick))
                return carry

            return lax.fori_loop(0, HALF // QUARTER, stats, done)

        lax.fori_loop(0, m // HALF, half, 0)


def score(hidden, weights, old, info, plan):
    m = hidden.shape[0]
    widths = [width for width, _ in plan]
    first = old is None
    vmem = pl.BlockSpec(memory_space=pltpu.VMEM)
    return pl.pallas_call(
        lambda *refs: score_body(plan, first, *refs),
        in_specs=[pl.BlockSpec(memory_space=pltpu.SMEM), vmem, *[any_spec()] * len(weights)]
        + ([] if first else [vmem]),
        out_specs=vmem,
        scratch_shapes=[
            pltpu.VMEM((HALF, max(widths)), jnp.float32),
            pltpu.SemaphoreType.DMA((len(weights),)),
            *[pltpu.VMEM((width, D), hidden.dtype) for width in widths],
        ],
        out_shape=jax.ShapeDtypeStruct((m, LANES), jnp.float32),
        cost_estimate=pl.CostEstimate(
            flops=2 * m * D * sum(widths), bytes_accessed=2 * (m + sum(widths)) * D, transcendentals=m * sum(widths)
        ),
        compiler_params=pltpu.CompilerParams(vmem_limit_bytes=24 << 20),
    )(info, hidden, *weights, *([] if first else [old]))


def around(n, k):
    return [(i, (i + k) % n) for i in range(n)]


def shards(head, hidden, targets):
    z, c = lax.axis_index("z"), lax.axis_index("c")
    block = lax.axis_index(("y", "x"))
    slabs = [lax.rem(z + 4 - j, 4) * 2 + lax.rem(c + e, 2) for e in range(2) for j in range(4)]
    mine = join(hidden, targets)
    every = lax.all_gather(mine, ("z", "y", "x"), axis=0, tiled=True)
    stats, flat, waiting, group = None, None, [], 0
    for width, off in zip(WIDTHS, STARTS):
        sent = cut(head, off, width)
        got = lax.all_to_all(sent, ("y", "x"), split_axis=0, concat_axis=0, tiled=True)
        got = got.reshape(TP * ROWS, width)
        flat, *pieces = turn(got, flat, z.reshape(1), off)
        for j in range(1, 4):
            pieces[j] = lax.ppermute(pieces[j], "z", around(4, j))
        other = []
        for j in range(4):
            other.append(lax.ppermute(pieces[j], "c", around(2, 1)))
        part = width // 4
        valid = min(width, BLOCK - off)
        waiting.append((pieces + other, block * BLOCK + off + z * part, valid - z * part, (part, valid < width)))
        if len(waiting) == GROUPS[group]:
            info = jnp.stack([*slabs, *[v for w in waiting for v in w[1:3]]]).astype(jnp.int32)
            stats = score(every, [p for w in waiting for p in w[0]], stats, info, [w[3] for w in waiting])
            waiting, group = [], group + 1
    table = stats[:, :3].reshape(64, 16, 3).transpose(0, 2, 1).reshape(64, 48)
    table = lax.all_to_all(table, ("z", "y", "x"), split_axis=0, concat_axis=0, tiled=True)
    table = table.reshape(64, 3, 16)
    peak = jnp.max(table[:, 0], axis=0)
    mass = jnp.sum(table[:, 1] * jnp.exp(table[:, 0] - peak), axis=0)
    norm = peak + jnp.log(mass)
    return flat.T, norm, jnp.sum(table[:, 2], axis=0) - norm


def solution(mesh):
    devices = Mesh(mesh.devices.reshape(4, 2, 4, 4), AXES)
    return jax.shard_map(
        shards,
        mesh=devices,
        in_specs=(P(AXES, None), P(AXES, None), P(AXES)),
        out_specs=(P(("z", "c"), ("y", "x")), P(AXES), P(AXES)),
        check_vma=False,
    )
```
